256 devices in a mesh: chan: 4 (over y), slab: 64 (over x, z, core).
Axes of the slice: x: 4, y: 4, z: 8, core: 2. Of those that a mesh axis runs over, the one named last changes fastest.
Arguments:
- flux: float32 [4, 4096, 128], P('chan', 'slab'), may hold values from -6 to 6
- offsets: int32 [4096, 128], P('slab'), may hold values from 0 to 8191
- counts: int32 [4096], P('slab'), may hold values from 96 to 128
- dest_owner: int32 [4096, 1], P('slab'), may hold values from 0 to 63; in each aligned block of 64 rows (0 to 63, 64 to 127, ...) at most 2 rows name the same one
- dest_tile: int32 [4096], P('slab'), may hold values from 0 to 31
- dirty: float32 [4, 4096, 4096], P('chan', 'slab'), may hold values from -60 to 60
- psf_real: float32 [4, 8192, 8192], P('chan', None, 'slab'), may hold values from -96 to 96
- psf_imag: float32 [4, 8192, 8192], P('chan', None, 'slab'), may hold values from -96 to 96
Outputs:
- residual: float32 [4, 4096, 4096], P('chan', 'slab')
- rms_values: float32 [4], replicated
- peak_values: float32 [4], replicated
The draws below stay inside these ranges and needn't reach their ends.
Inputs may be any that keep to these rules, and one draw needn't show every extreme that they name: `dest_owner`: among the 64 blocks of one device (aligned blocks of rows) at most 2 name the same owner, a bound that some device reaches. `counts`: slots at or beyond a block's count hold no component.
All inputs are finite; a program needn't handle non-finite values.
Results may differ from the reference program's by a relative error of at most 0.00005.
Values sent between devices are 32-bit elements; how exact they have to be, the bound alone decides.
A program may use at most 128 MiB of HBM per device.

```python
import math
import jax
import jax.numpy as jnp
import numpy as np
from jax import lax

IMG = 4096
COMP = 128
TILE_R = 64
TILE_C = 128
BLK_DEV = 64
PAD = 8192
SEND = 2
TILES_OWN = 32
CHANNELS = 4
BLOCKS = 4096
N_SLAB = 64


def draw_dirty(key, part):
    key_base = jax.random.fold_in(key, 11)
    key_cols = jax.random.fold_in(key, 12)
    row_frac = jnp.arange(IMG, dtype=jnp.float32)[:, None] / IMG
    col_frac = jax.random.uniform(key_cols, (1, IMG), jnp.float32)
    base_noise = jnp.clip(jax.random.normal(key_base, (CHANNELS, IMG, IMG), jnp.float32), -6.0, 6.0)
    return 0.3 * base_noise * 10.0 ** row_frac * 10.0 ** (0.5 * col_frac)


def set_ends(result, rng, low, top_value):
    shape = result.shape
    place = [jax.random.randint(jax.random.fold_in(rng, axis), (), 0, shape[axis]) for axis in range(len(shape))]
    result = result.at[tuple(place)].set(low)
    longest = shape.index(max(shape))
    place[longest] = (place[longest] + 1) % shape[longest]
    return result.at[tuple(place)].set(top_value)


def block_levels(stream_key, dims, shards, smallest, top_value):
    factor_of, own = 1.0, jax.random.fold_in(stream_key, 6)
    for position, shards_of in shards:
        draws = jnp.exp(jax.random.uniform(jax.random.fold_in(own, position), (shards_of,), jnp.float32, smallest / len(shards), top_value / len(shards)))
        factor_of = factor_of * jnp.repeat(draws, dims[position] // shards_of).reshape([-1 if axis == position else 1 for axis in range(len(dims))])
    return factor_of


def deal_out(key, own, number, rows, number_of, top, reach, slope):
    order = jax.random.permutation(key, number_of)
    heavy_load, usual = load_shares(number_of, rows * top, reach, slope, True), load_shares(number_of, rows * top, reach, slope, False)
    places = jnp.arange(number_of)

    def named(tallies, rotation):
        used = int((tallies > 0).sum())
        fixed = max(1, used // 4)
        passed = fixed + (places - fixed + rotation * (used - fixed)) % max(1, number_of - fixed)
        return jnp.zeros((number_of,), jnp.int32).at[order[jnp.where(places < fixed, places, passed)]].set(jnp.asarray(tallies, jnp.int32))

    tallies = jnp.where(number % 4 == 0, named(heavy_load, number // 4), named(usual, number - number // 4 - 1))
    mixed = jax.random.permutation(jax.random.fold_in(own, 3), number_of)
    donor, receiver = mixed[0:number_of // 2 * 2:2], mixed[1:number_of // 2 * 2:2]
    room = jnp.minimum(tallies[donor] - 1, reach - tallies[receiver]) // 2
    room = jnp.where((donor == order[0]) | (receiver == order[0]) | (tallies[receiver] == 0), 0, jnp.maximum(room, 0))
    passed = jax.random.randint(jax.random.fold_in(own, 4), (number_of // 2,), 0, 1 << 20) % (room + 1)
    tallies = tallies.at[donor].add(-passed).at[receiver].add(passed)
    items = jnp.searchsorted(jnp.cumsum(tallies), jnp.arange(rows * top), side="right").astype(jnp.int32)
    listing = items.reshape(top, rows).T
    listing = listing[jax.random.permutation(jax.random.fold_in(own, 1), rows)]
    rotation = jax.random.randint(jax.random.fold_in(own, 2), (rows, 1), 0, top)
    return jnp.take_along_axis(listing, (jnp.arange(top)[None, :] + rotation) % top, axis=1)


def load_shares(amount, total, most, lean, full):
    portions = [(1 << 20) // math.isqrt(standing ** lean) + 1 for standing in range(1, amount + 1)]
    largest = most if full else min(most, max(-(-total // amount), total * portions[0] // sum(portions)))
    least = 1 if total - largest >= amount - 1 else 0
    holding, spare = [largest] + [least] * (amount - 1), total - largest - least * (amount - 1)
    while spare > 0:
        movable = [i for i in range(1, amount) if holding[i] < largest] or [i for i in range(1, amount) if holding[i] < most]
        whole, remaining = sum([portions[i] for i in movable]), spare
        for i in movable:
            addition = min(most - holding[i], max(1, remaining * portions[i] // whole), spare)
            holding[i] = holding[i] + addition
            spare = spare - addition
    return np.array(holding)


def noise(key, dims, spread, bound, shards=(), kind=jnp.bfloat16):
    result = jax.random.normal(key, dims, jnp.float32) * spread
    if len(shards) > 0:
        result = block_levels(key, dims, shards, -0.22, 0.18) * result
    return jnp.clip(result, min=-bound, max=bound).astype(kind)


def setup_inputs(seed: int = 0) -> dict:
    streams_of = jax.random.split(jax.random.key(seed), 9)
    flux = noise(streams_of[0], (CHANNELS, BLOCKS, COMP), 1.0, 6.0, ((0, 4), (1, 64)), jnp.float32)
    offsets = set_ends(jax.random.randint(streams_of[1], (BLOCKS, COMP), 0, TILE_R * TILE_C), jax.random.fold_in(streams_of[1], 1), 0, (TILE_R * TILE_C) - 1).astype(jnp.int32)
    counts = set_ends(jax.random.randint(streams_of[2], (BLOCKS,), COMP * 3 // 4, COMP + 1), jax.random.fold_in(streams_of[2], 1), COMP * 3 // 4, COMP).astype(jnp.int32)
    dest_owner_keys = jax.random.split(jax.random.fold_in(streams_of[3], 1), BLOCKS // BLK_DEV)
    dest_owner_turns = jax.random.permutation(jax.random.fold_in(streams_of[3], 3), BLOCKS // BLK_DEV)
    dest_owner = jax.vmap(lambda own, number: deal_out(jax.random.fold_in(streams_of[3], 2), own, number, BLK_DEV, N_SLAB, 1, SEND, 2))(dest_owner_keys, dest_owner_turns).reshape((BLOCKS, 1))
    dest_tile = set_ends(jax.random.randint(streams_of[4], (BLOCKS,), 0, TILES_OWN), jax.random.fold_in(streams_of[4], 1), 0, TILES_OWN - 1).astype(jnp.int32)
    dirty = draw_dirty(jax.random.fold_in(streams_of[8], 71), 0)
    psf_real = noise(streams_of[6], (CHANNELS, PAD, PAD), (PAD // 512), 96.0, ((0, 4), (2, 64)), jnp.float32)
    psf_imag = noise(streams_of[7], (CHANNELS, PAD, PAD), (PAD // 512), 96.0, ((0, 4), (2, 64)), jnp.float32)
    return {"flux": flux, "offsets": offsets, "counts": counts, "dest_owner": dest_owner, "dest_tile": dest_tile, "dirty": dirty, "psf_real": psf_real, "psf_imag": psf_imag}


def reference(flux, offsets, counts, dest_owner, dest_tile, dirty, psf_real, psf_imag):
    rows_dev = IMG // N_SLAB
    across = IMG // TILE_C
    tile_row = dest_tile // across
    tile_col = dest_tile % across
    owner_ids = dest_owner[:, 0]
    pixels = ((owner_ids[:, None] * rows_dev + tile_row[:, None] * TILE_R + offsets // TILE_C) * IMG + tile_col[:, None] * TILE_C + offsets % TILE_C).reshape(-1).astype(jnp.int32)
    live_mask = jnp.arange(COMP, dtype=jnp.int32)[None, :] < counts[:, None]
    weights = jnp.where(live_mask[None], flux, jnp.zeros_like(flux)).reshape(CHANNELS, -1)

    def one_channel(members):
        weight, dirty_part, spec_real, spec_imag = members
        model_image = jnp.zeros((IMG * IMG,), flux.dtype).at[pixels].add(weight).reshape(IMG, IMG)
        spectrum = jnp.fft.fft2(model_image, s=(PAD, PAD))
        convolved = jnp.fft.ifft2(spectrum * lax.complex(spec_real, spec_imag))
        residual = dirty_part - jnp.real(convolved[:IMG, :IMG])
        return (residual, jnp.sqrt(jnp.mean(residual * residual)), jnp.max(jnp.abs(residual)))
    residual, rms_values, peak_values = lax.map(one_channel, (weights, dirty, psf_real, psf_imag))
    return (residual, rms_values, peak_values)
```

```python
import functools
import math

import jax
import jax.numpy as jnp
import numpy as np
from jax import lax
from jax.experimental import pallas as pl
from jax.experimental.pallas import tpu as pltpu
from jax.sharding import Mesh
from jax.sharding import PartitionSpec as P

TILE_R = 64
TILE_C = 128
SLAB = ("slab_0", "slab_1", "slab_2")
ROWS = 64
COLS = 128
PEERS = 64
LENGTH = 8192
TILES = 32

BF = jnp.bfloat16
F32 = jnp.float32


def halves(table):
    table = np.asarray(table, np.float32)
    high = table.astype(jnp.bfloat16)
    low = (table - high.astype(np.float32)).astype(jnp.bfloat16)
    return high, low


def turns(first, second, length):
    return 2.0 * math.pi * (np.outer(first, second) % length) / length


def row_tables():
    j, tc, cc, d = np.arange(COLS), np.arange(TILES), np.arange(TILE_C), np.arange(PEERS)
    angle = turns(j, tc, 64)
    high, low = halves(np.concatenate([np.cos(angle), -np.sin(angle)], axis=0))
    first = np.concatenate([high, high, low], axis=1)
    angle = turns(j, cc, LENGTH)
    tw_re, tw_im = np.cos(angle).astype(np.float32), (-np.sin(angle)).astype(np.float32)
    angle = turns(d, cc, 64)
    block = np.stack(
        [
            np.concatenate([np.cos(angle), np.sin(angle)], axis=1),
            np.concatenate([-np.sin(angle), np.cos(angle)], axis=1),
        ],
        axis=1,
    ).reshape(2 * PEERS, 2 * TILE_C)
    high, low = halves(block)
    second = np.concatenate([high, low], axis=0)
    return first, tw_re, tw_im, second


def column_tables():
    a, k, m, b = np.arange(64), np.arange(128), np.arange(64), np.arange(64)
    angle = turns(k, a, 128)
    c, s = np.cos(angle), np.sin(angle)
    first = np.stack([np.stack([c, s], axis=2), np.stack([-s, c], axis=2)], axis=1)
    first_hi, first_lo = halves(first.reshape(256, 128))
    angle = turns(m, b, 64)
    c, s = np.cos(angle), np.sin(angle)
    second = np.block([[c, s], [-s, c]]).astype(np.float32)
    second_turn = np.block([[-s, c], [-c, -s]]).astype(np.float32)
    angle = turns(k, b, LENGTH)
    phase = np.stack([np.tile(np.cos(angle), (1, 2)), np.tile(np.sin(angle), (1, 2))], axis=1)
    angle = turns(b, m, 64)
    c, s = np.cos(angle), np.sin(angle)
    third_hi, third_lo = halves(np.block([[c, -s], [s, c]]))
    third = np.concatenate([third_hi, third_lo], axis=1)
    angle = turns(a, k, 128)
    c, s = np.cos(angle) * 2.0**-26, np.sin(angle) * 2.0**-26
    fourth = np.stack([np.stack([c, -s], axis=2), np.stack([s, c], axis=2)], axis=1)
    fourth_turn = np.stack([np.stack([-s, -c], axis=2), np.stack([c, -s], axis=2)], axis=1)
    angle = np.repeat(turns(b, k, LENGTH), 2, axis=1)
    last_phase = np.stack([np.cos(angle), np.sin(angle)], axis=1)
    return (
        np.concatenate([first_hi, first_hi], axis=1),
        first_lo,
        second,
        second_turn,
        phase.astype(np.float32),
        third,
        fourth.reshape(128, 256).astype(np.float32),
        fourth_turn.reshape(128, 256).astype(np.float32),
        last_phase.astype(np.float32),
    )


def inverse_tables():
    d, q, j, n2, n1 = np.arange(64), np.arange(64), np.arange(128), np.arange(128), np.arange(32)
    angle = turns(q, d, 64)
    c, s = np.cos(angle), np.sin(angle)
    first = np.concatenate(
        [
            np.stack([c, -s], axis=2).reshape(64, 128),
            np.stack([s, c], axis=2).reshape(64, 128),
        ],
        axis=0,
    )
    first_hi, first_lo = halves(first)
    angle = turns(n2, j, LENGTH)
    tw_re, tw_im = np.cos(angle).astype(np.float32), np.sin(angle).astype(np.float32)
    angle = turns(n1, j, 64)
    high, low = halves(np.concatenate([np.cos(angle), -np.sin(angle)], axis=1))
    return (
        np.concatenate([first_hi, first_hi], axis=1),
        first_lo,
        tw_re,
        tw_im,
        np.concatenate([high, low], axis=0),
    )


def split(value):
    high = value.astype(BF)
    low = (value - high.astype(F32)).astype(BF)
    return high, low


def mm(first, second):
    return jnp.dot(first, second, preferred_element_type=F32)


def mm_nt(first, second):
    return lax.dot_general(
        first, second, (((1,), (1,)), ((), ())), preferred_element_type=F32
    )


GROUP = 4


def rows_kernel(tile_ref, got_ref, first_ref, twr_ref, twi_ref, second_ref, out_ref, image):
    step = pl.program_id(0)
    blocks = got_ref.shape[0] // 2

    @pl.when(step == 0)
    def _():
        image[...] = jnp.zeros_like(image)
        row_ids = lax.broadcasted_iota(jnp.int32, (TILE_R, 128), 0)
        col_ids = lax.broadcasted_iota(jnp.int32, (TILE_C, 128), 0)

        def body(it, carry):
            tiles = []
            both = got_ref[pl.ds(pl.multiple_of(it * 2 * GROUP, 2 * GROUP), 2 * GROUP), :]
            for g in range(GROUP):
                place = both[2 * g : 2 * g + 1].astype(jnp.int32)
                flux = both[2 * g + 1 : 2 * g + 2]
                row = (place >> 7) & (TILE_R - 1)
                col = place & (TILE_C - 1)
                high = flux.astype(BF).astype(F32)
                low = flux - high
                here = row_ids == row
                lhs = jnp.concatenate(
                    [jnp.where(here, high, 0.0), jnp.where(here, low, 0.0)], axis=0
                ).astype(BF)
                rhs = jnp.where(col_ids == col, 1.0, 0.0).astype(BF)
                both_parts = mm_nt(lhs, rhs)
                tiles.append(both_parts[:TILE_R] + both_parts[TILE_R:])
            for g in range(GROUP):
                at = pl.ds(pl.multiple_of(tile_ref[it * GROUP + g] * TILE_R, TILE_R), TILE_R)
                image[at, :] += tiles[g]
            return carry

        lax.fori_loop(0, blocks // GROUP, body, 0)

    rows = out_ref.shape[1]
    out = out_ref.reshape(2 * PEERS * rows, COLS)
    for pair in range(rows // 2):
        parts = []
        for e in range(2):
            x = image[pl.ds(step * rows + 2 * pair + e, TILES, stride=TILE_R), :]
            high, low = split(x)
            parts.append(jnp.concatenate([high, low, high], axis=0))
        partial = mm(first_ref[...], jnp.concatenate(parts, axis=1))
        turned = []
        for e in range(2):
            re = partial[:COLS, e * TILE_C : (e + 1) * TILE_C]
            im = partial[COLS:, e * TILE_C : (e + 1) * TILE_C]
            turned.append(
                jnp.concatenate(
                    [
                        re * twr_ref[...] - im * twi_ref[...],
                        re * twi_ref[...] + im * twr_ref[...],
                    ],
                    axis=1,
                )
            )
        high, low = split(jnp.concatenate(turned, axis=0))
        full = mm_nt(second_ref[...], high)
        part = mm_nt(second_ref[: 2 * PEERS], low)
        result = full[: 2 * PEERS] + full[2 * PEERS :] + part
        for e in range(2):
            out[pl.ds(2 * pair + e, 2 * PEERS, stride=rows), :] = result[
                :, e * COLS : (e + 1) * COLS
            ]


def whole(shape):
    return pl.BlockSpec(shape, lambda *_: (0,) * len(shape))


def forward_rows(tiles, got, rows=8):
    first, twr, twi, second = row_tables()
    return pl.pallas_call(
        rows_kernel,
        out_shape=jax.ShapeDtypeStruct((2 * PEERS, ROWS, COLS), F32),
        grid=(ROWS // rows,),
        in_specs=[
            pl.BlockSpec(memory_space=pltpu.SMEM),
            whole(got.shape),
            whole(first.shape),
            whole(twr.shape),
            whole(twi.shape),
            whole(second.shape),
        ],
        out_specs=pl.BlockSpec((2 * PEERS, rows, COLS), lambda i: (0, i, 0)),
        scratch_shapes=[pltpu.VMEM((TILES * TILE_R, TILE_C), F32)],
        name="rows",
    )(tiles, got, jnp.asarray(first), jnp.asarray(twr), jnp.asarray(twi), jnp.asarray(second))


STEPS = 8


def columns_kernel(
    x_ref,
    pr_ref,
    pi_ref,
    first_ref,
    first_lo_ref,
    second_ref,
    second_turn_ref,
    phase_ref,
    third_ref,
    fourth_ref,
    fourth_turn_ref,
    last_phase_ref,
    out_ref,
    held,
):
    step = pl.program_id(0)
    rows = x_ref.shape[1]
    per = pr_ref.shape[1]

    @pl.when(step < STEPS)
    def _():
        x = x_ref.reshape(128 * rows, COLS)
        for pair in range(rows // 2):
            values = jnp.concatenate(
                [x[pl.ds(2 * pair + e, 128, stride=rows), :] for e in range(2)], axis=1
            )
            high, low = split(values)
            both = jnp.concatenate([high, low], axis=0)
            result = mm(first_ref[...], both) + mm(first_lo_ref[...], high)
            for e in range(2):
                at = pl.multiple_of((step * rows + 2 * pair + e) * 256, 256)
                held[pl.ds(at, 256), :] = result[:, e * COLS : (e + 1) * COLS]

    @pl.when(jnp.logical_and(step >= STEPS, step < 2 * STEPS))
    def _():
        pr = pr_ref.reshape(64 * per, COLS)
        pi = pi_ref.reshape(64 * per, COLS)

        def body(i, carry):
            k = (step - STEPS) * per + i
            table = (
                second_ref[...] * phase_ref[k, 0:1, :] + second_turn_ref[...] * phase_ref[k, 1:2, :]
            )
            table_hi, table_lo = split(table)
            values = jnp.concatenate(
                [held[pl.ds(2 * k + s, 64, stride=256), :] for s in range(2)], axis=0
            )
            high, low = split(values)
            spectrum = mm(
                jnp.concatenate([table_hi, table_lo], axis=1),
                jnp.concatenate([high, high], axis=0),
            ) + mm(table_hi, low)
            re, im = spectrum[:64], spectrum[64:]
            psf_re = pr[pl.ds(i, 64, stride=per), :]
            psf_im = pi[pl.ds(i, 64, stride=per), :]
            filtered = jnp.concatenate(
                [re * psf_re - im * psf_im, re * psf_im + im * psf_re], axis=0
            )
            high, low = split(filtered)
            third = third_ref[...]
            result = mm(third, jnp.concatenate([high, high], axis=0)) + mm(third[:, :128], low)
            for s in range(2):
                held[pl.ds(2 * k + s, 64, stride=256), :] = result[64 * s : 64 * s + 64]
            return carry

        lax.fori_loop(0, per, body, 0, unroll=4)

    @pl.when(step >= 2 * STEPS)
    def _():
        out = out_ref.reshape(128 * rows, COLS)
        for pair in range(rows // 2):
            for e in range(2):
                row = (step - 2 * STEPS) * rows + 2 * pair + e
                table = (
                    fourth_ref[...] * last_phase_ref[row, 0:1, :]
                    + fourth_turn_ref[...] * last_phase_ref[row, 1:2, :]
                )
                table_hi, table_lo = split(table)
                at = pl.multiple_of(row * 256, 256)
                high, low = split(held[pl.ds(at, 256), :])
                full = mm(jnp.concatenate([table_hi, table_lo], axis=0), high)
                result = full[:128] + full[128:] + mm(table_hi, low)
                out[pl.ds(2 * pair + e, 128, stride=rows), :] = result


def columns(values, psf_re, psf_im):
    tables = column_tables()
    rows = ROWS // STEPS
    per = 128 // STEPS
    psf_re = psf_re.reshape(64, 128, COLS)
    psf_im = psf_im.reshape(64, 128, COLS)

    def psf_at(i):
        return (0, jnp.clip(i - STEPS, 0, STEPS - 1), 0)

    return pl.pallas_call(
        columns_kernel,
        out_shape=jax.ShapeDtypeStruct((128, ROWS, COLS), F32),
        grid=(3 * STEPS,),
        in_specs=[
            pl.BlockSpec((128, rows, COLS), lambda i: (0, jnp.minimum(i, STEPS - 1), 0)),
            pl.BlockSpec((64, per, COLS), psf_at),
            pl.BlockSpec((64, per, COLS), psf_at),
        ]
        + [whole(t.shape) for t in tables],
        out_specs=pl.BlockSpec(
            (128, rows, COLS), lambda i: (0, jnp.maximum(i - 2 * STEPS, 0), 0)
        ),
        scratch_shapes=[pltpu.VMEM((64 * 256, COLS), F32)],
        name="columns",
    )(values, psf_re, psf_im, *[jnp.asarray(t) for t in tables])


def inverse_kernel(
    y_ref, dirty_ref, first_ref, first_lo_ref, twr_ref, twi_ref, last_ref, out_ref, stat_ref, smear
):
    step = pl.program_id(0)
    rows = y_ref.shape[1]
    y = y_ref.reshape(128 * rows, COLS)
    for pair in range(rows // 2):
        values = jnp.concatenate(
            [y[pl.ds(2 * pair + e, 128, stride=rows), :] for e in range(2)], axis=1
        )
        high, low = split(values)
        partial = mm(first_ref[...], jnp.concatenate([high, low], axis=0)) + mm(
            first_lo_ref[...], high
        )
        turned = []
        for e in range(2):
            re = partial[:64, e * COLS : (e + 1) * COLS]
            im = partial[64:, e * COLS : (e + 1) * COLS]
            re = jnp.concatenate([re, re], axis=0)
            im = jnp.concatenate([im, im], axis=0)
            turned.append(
                jnp.concatenate(
                    [
                        re * twr_ref[...] - im * twi_ref[...],
                        re * twi_ref[...] + im * twr_ref[...],
                    ],
                    axis=1,
                )
            )
        high, low = split(jnp.concatenate(turned, axis=0))
        full = mm_nt(last_ref[...], high)
        result = full[:TILES] + full[TILES:] + mm_nt(last_ref[:TILES], low)
        for e in range(2):
            smear[pl.ds(2 * pair + e, TILES, stride=rows), :] = result[
                :, e * TILE_C : (e + 1) * TILE_C
            ]
    squares = jnp.zeros((rows, TILE_C), F32)
    peaks = jnp.zeros((rows, TILE_C), F32)
    for t in range(TILES):
        lanes = slice(t * TILE_C, (t + 1) * TILE_C)
        rest = dirty_ref[:, lanes] - smear[t * rows : (t + 1) * rows, :]
        out_ref[:, lanes] = rest
        squares += rest * rest
        peaks = jnp.maximum(peaks, jnp.abs(rest))

    @pl.when(step == 0)
    def _():
        stat_ref[...] = jnp.zeros_like(stat_ref)

    stat_ref[0:8, :] += squares
    stat_ref[8:16, :] = jnp.maximum(stat_ref[8:16, :], peaks)


def inverse_rows(values, dirty):
    tables = inverse_tables()
    rows = 8
    width = dirty.shape[1]
    return pl.pallas_call(
        inverse_kernel,
        out_shape=(
            jax.ShapeDtypeStruct((ROWS, width), F32),
            jax.ShapeDtypeStruct((16, TILE_C), F32),
        ),
        grid=(ROWS // rows,),
        in_specs=[
            pl.BlockSpec((128, rows, COLS), lambda i: (0, i, 0)),
            pl.BlockSpec((rows, width), lambda i: (i, 0)),
        ]
        + [whole(t.shape) for t in tables],
        out_specs=(
            pl.BlockSpec((rows, width), lambda i: (i, 0)),
            pl.BlockSpec((16, TILE_C), lambda i: (0, 0)),
        ),
        scratch_shapes=[pltpu.VMEM((TILES * rows, TILE_C), F32)],
        name="inverse",
    )(values, dirty, *[jnp.asarray(t) for t in tables])


def boxes(flux, offsets, counts, dest_owner, dest_tile):
    blocks, slots = offsets.shape
    live = jnp.arange(slots, dtype=jnp.int32)[None, :] < counts[:, None]
    weights = jnp.where(live, flux, 0.0)
    places = (dest_tile[:, None] * (TILE_R * TILE_C) + offsets).astype(F32)
    payload = jnp.concatenate([places, weights], axis=1)
    owner = dest_owner[:, 0]
    ids = jnp.arange(blocks, dtype=jnp.int32)
    same = (owner[:, None] == owner[None, :]) & (ids[None, :] < ids[:, None])
    rank = jnp.sum(same.astype(jnp.int32), axis=1)
    slot = owner * 2 + rank
    marks = (slot[None, :] == jnp.arange(2 * PEERS, dtype=jnp.int32)[:, None]).astype(F32)
    box = jnp.dot(marks, payload, precision=lax.Precision.HIGHEST)
    return box.reshape(PEERS, 4, slots)


def on_device(flux, offsets, counts, dest_owner, dest_tile, dirty, psf_real, psf_imag):
    box = boxes(flux[0], offsets, counts, dest_owner, dest_tile)
    got = lax.all_to_all(box, SLAB, split_axis=0, concat_axis=0, tiled=True)
    tiles = got.reshape(2 * PEERS, 2, -1)[:, 0, 0].astype(jnp.int32) // (TILE_R * TILE_C)
    rows = forward_rows(tiles, got.reshape(4 * PEERS, -1))
    rows = rows.reshape(PEERS, 2, ROWS, COLS)
    turned = lax.all_to_all(rows, SLAB, split_axis=0, concat_axis=0, tiled=True)
    back = columns(turned.reshape(2 * PEERS, ROWS, COLS), psf_real[0], psf_imag[0])
    back = back.reshape(PEERS, 2, ROWS, COLS)
    home = lax.all_to_all(back, SLAB, split_axis=0, concat_axis=0, tiled=True)
    residual, stats = inverse_rows(home.reshape(2 * PEERS, ROWS, COLS), dirty[0])
    own = jnp.stack([jnp.sum(stats[:8]), jnp.max(stats[8:])])
    every = lax.all_gather(own[None], ("chan",) + SLAB, axis=0, tiled=True)
    every = every.reshape(-1, PEERS, 2)
    pixel_total = PEERS * dirty.shape[1] * dirty.shape[2]
    rms_values = jnp.sqrt(jnp.sum(every[:, :, 0], axis=1) / pixel_total)
    peak_values = jnp.max(every[:, :, 1], axis=1)
    return residual[None], rms_values, peak_values


def solution(mesh):
    torus = Mesh(
        mesh.devices.reshape(mesh.shape["chan"], 4, 8, 2), ("chan", "slab_0", "slab_1", "slab_2")
    )
    in_specs = (
        P("chan", SLAB, None),
        P(SLAB, None),
        P(SLAB),
        P(SLAB, None),
        P(SLAB),
        P("chan", SLAB, None),
        P("chan", None, SLAB),
        P("chan", None, SLAB),
    )
    out_specs = (P("chan", SLAB, None), P(), P())
    return jax.shard_map(
        on_device, mesh=torus, in_specs=in_specs, out_specs=out_specs, check_vma=False
    )
```

```python
import functools
import math

import jax
import jax.numpy as jnp
import numpy as np
from jax import lax
from jax.experimental import pallas as pl
from jax.experimental.pallas import tpu as pltpu
from jax.sharding import Mesh
from jax.sharding import PartitionSpec as P

TILE_R = 64
TILE_C = 128
SLAB = ("slab_0", "slab_1", "slab_2")
ROWS = 64
COLS = 128
PEERS = 64
LENGTH = 8192
TILES = 32

BF = jnp.bfloat16
F32 = jnp.float32


def halves(table):
    table = np.asarray(table, np.float32)
    high = table.astype(jnp.bfloat16)
    low = (table - high.astype(np.float32)).astype(jnp.bfloat16)
    return high, low


def turns(first, second, length):
    return 2.0 * math.pi * (np.outer(first, second) % length) / length


def row_tables():
    j, tc, cc, d = np.arange(COLS), np.arange(TILES), np.arange(TILE_C), np.arange(PEERS)
    angle = turns(j, tc, 64)
    high, low = halves(np.concatenate([np.cos(angle), -np.sin(angle)], axis=0))
    first = np.concatenate([high, high, low], axis=1)
    angle = turns(j, cc, LENGTH)
    tw_re, tw_im = np.cos(angle).astype(np.float32), (-np.sin(angle)).astype(np.float32)
    d = d.reshape(4, 8, 2)[:, np.arange(12) % 8].transpose(1, 0, 2).reshape(-1)
    angle = turns(d, cc, 64)
    block = np.stack(
        [
            np.concatenate([np.cos(angle), np.sin(angle)], axis=1),
            np.concatenate([-np.sin(angle), np.cos(angle)], axis=1),
        ],
        axis=1,
    ).reshape(-1, 2 * TILE_C)
    return first, tw_re, tw_im, *halves(block)


def column_tables():
    a, k, m, b = np.arange(64), np.arange(128), np.arange(64), np.arange(64)
    angle = turns(k, a, 128)
    c, s = np.cos(angle), np.sin(angle)
    first = np.stack([np.stack([c, s], axis=2), np.stack([-s, c], axis=2)], axis=1)
    first_hi, first_lo = halves(first.reshape(256, 128))
    angle = turns(m, b, 64)
    c, s = np.cos(angle), np.sin(angle)
    second = np.block([[c, s], [-s, c]]).astype(np.float32)
    second_turn = np.block([[-s, c], [-c, -s]]).astype(np.float32)
    angle = turns(k, b, LENGTH)
    phase = np.stack([np.tile(np.cos(angle), (1, 2)), np.tile(np.sin(angle), (1, 2))], axis=1)
    angle = turns(b, m, 64)
    c, s = np.cos(angle), np.sin(angle)
    third_hi, third_lo = halves(np.block([[c, -s], [s, c]]))
    third = np.concatenate([third_hi, third_lo], axis=1)
    angle = turns(a, k, 128)
    c, s = np.cos(angle) * 2.0**-26, np.sin(angle) * 2.0**-26
    fourth = np.stack([np.stack([c, -s], axis=2), np.stack([s, c], axis=2)], axis=1)
    fourth_turn = np.stack([np.stack([-s, -c], axis=2), np.stack([c, -s], axis=2)], axis=1)
    angle = np.repeat(turns(b, k, LENGTH), 2, axis=1)
    last_phase = np.stack([np.cos(angle), np.sin(angle)], axis=1)
    return (
        np.concatenate([first_hi, first_hi], axis=1),
        first_lo,
        second,
        second_turn,
        phase.astype(np.float32),
        third,
        fourth.reshape(128, 256).astype(np.float32),
        fourth_turn.reshape(128, 256).astype(np.float32),
        last_phase.astype(np.float32),
    )


def inverse_tables():
    d, q, j, n2, n1 = np.arange(64), np.arange(64), np.arange(128), np.arange(128), np.arange(32)
    angle = turns(q, d, 64)
    c, s = np.cos(angle), np.sin(angle)
    first = np.concatenate(
        [
            np.stack([c, -s], axis=2).reshape(64, 128),
            np.stack([s, c], axis=2).reshape(64, 128),
        ],
        axis=0,
    )
    first_hi, first_lo = halves(first)
    angle = turns(n2, j, LENGTH)
    tw_re, tw_im = np.cos(angle).astype(np.float32), np.sin(angle).astype(np.float32)
    angle = turns(n1, j, 64)
    high, low = halves(np.concatenate([np.cos(angle), -np.sin(angle)], axis=1))
    return (
        np.concatenate([first_hi, first_hi], axis=1),
        first_lo,
        tw_re,
        tw_im,
        np.concatenate([high, low], axis=0),
    )


def split(value):
    high = value.astype(BF)
    low = (value - high.astype(F32)).astype(BF)
    return high, low


def mm(first, second):
    return jnp.dot(first, second, preferred_element_type=F32)


def mm_nt(first, second):
    return lax.dot_general(
        first, second, (((1,), (1,)), ((), ())), preferred_element_type=F32
    )


GROUP = 4


def rows_kernel(
    tile_ref, got_ref, first_ref, twr_ref, twi_ref, high_ref, low_ref, own_ref, far_ref, image
):
    step = pl.program_id(0)
    blocks = got_ref.shape[0] // 2
    rows = own_ref.shape[1]
    z = tile_ref[blocks]

    @pl.when(step == 0)
    def _():
        image[...] = jnp.zeros_like(image)
        row_ids = lax.broadcasted_iota(jnp.int32, (TILE_R, 128), 0)
        col_ids = lax.broadcasted_iota(jnp.int32, (TILE_C, 128), 0)

        def body(it, carry):
            tiles = []
            both = got_ref[pl.ds(pl.multiple_of(it * 2 * GROUP, 2 * GROUP), 2 * GROUP), :]
            for g in range(GROUP):
                place = both[2 * g : 2 * g + 1].astype(jnp.int32)
                flux = both[2 * g + 1 : 2 * g + 2]
                row = (place >> 7) & (TILE_R - 1)
                col = place & (TILE_C - 1)
                high = flux.astype(BF).astype(F32)
                low = flux - high
                here = row_ids == row
                lhs = jnp.concatenate(
                    [jnp.where(here, high, 0.0), jnp.where(here, low, 0.0)], axis=0
                ).astype(BF)
                rhs = jnp.where(col_ids == col, 1.0, 0.0).astype(BF)
                both_parts = mm_nt(lhs, rhs)
                tiles.append(both_parts[:TILE_R] + both_parts[TILE_R:])
            for g in range(GROUP):
                at = pl.ds(pl.multiple_of(tile_ref[it * GROUP + g] * TILE_R, TILE_R), TILE_R)
                image[at, :] += tiles[g]
            return carry

        lax.fori_loop(0, blocks // GROUP, body, 0)

    def chunk(base, reach, out_ref):
        many = (2 * reach + 1) * 16
        out = out_ref.reshape(many * rows, COLS)
        at = pl.ds(pl.multiple_of(lax.rem(z + 8 - reach, 8) * 16, 16), many)
        table_hi, table_lo = high_ref[at, :], low_ref[at, :]
        table = jnp.concatenate([table_hi, table_lo], axis=0)
        for pair in range(rows // 2):
            parts = []
            for e in range(2):
                x = image[pl.ds(base + 2 * pair + e, TILES, stride=TILE_R), :]
                high, low = split(x)
                parts.append(jnp.concatenate([high, low, high], axis=0))
            partial = mm(first_ref[...], jnp.concatenate(parts, axis=1))
            turned = []
            for e in range(2):
                re = partial[:COLS, e * TILE_C : (e + 1) * TILE_C]
                im = partial[COLS:, e * TILE_C : (e + 1) * TILE_C]
                turned.append(
                    jnp.concatenate(
                        [
                            re * twr_ref[...] - im * twi_ref[...],
                            re * twi_ref[...] + im * twr_ref[...],
                        ],
                        axis=1,
                    )
                )
            high, low = split(jnp.concatenate(turned, axis=0))
            full = mm_nt(table, high)
            result = full[:many] + full[many:] + mm_nt(table_hi, low)
            for e in range(2):
                out[pl.ds(2 * pair + e, many, stride=rows), :] = result[
                    :, e * COLS : (e + 1) * COLS
                ]

    chunks = ROWS // rows

    @pl.when(step < chunks)
    def _():
        chunk(step * rows, 2, own_ref)

    @pl.when(step >= chunks)
    def _():
        chunk(TILES * TILE_R + (step - chunks) * rows, 1, far_ref)


def whole(shape):
    return pl.BlockSpec(shape, lambda *_: (0,) * len(shape))


def forward_rows(tiles, got, rows=8):
    tables = row_tables()
    chunks = ROWS // rows
    return pl.pallas_call(
        rows_kernel,
        out_shape=(
            jax.ShapeDtypeStruct((80, ROWS, COLS), F32),
            jax.ShapeDtypeStruct((48, ROWS, COLS), F32),
        ),
        grid=(2 * chunks,),
        in_specs=[
            pl.BlockSpec(memory_space=pltpu.SMEM),
            whole(got.shape),
        ]
        + [whole(t.shape) for t in tables],
        out_specs=(
            pl.BlockSpec((80, rows, COLS), lambda i: (0, jnp.minimum(i, chunks - 1), 0)),
            pl.BlockSpec((48, rows, COLS), lambda i: (0, jnp.maximum(i - chunks, 0), 0)),
        ),
        scratch_shapes=[pltpu.VMEM((2 * TILES * TILE_R, TILE_C), F32)],
        name="rows",
    )(tiles, got, *[jnp.asarray(t) for t in tables])


def spread_kernel(own_ref, far_ref, out_ref, send_sem, recv_sem, local_sem):
    x, z, core = (lax.axis_index(a) for a in SLAB)

    def peer(i):
        order = i // 8
        dz = (order + 1) // 2 * (1 - 2 * (1 - order % 2) * jnp.minimum(order, 1))
        return (x + i // 2 % 4) % 4, (z + 8 + dz) % 8, (core + i) % 2, dz

    def copy(i, far):
        px, pz, pc, dz = peer(i)
        reach = 1 if far else 2
        src = far_ref if far else own_ref
        block = ((dz + reach) * 4 + px) * 2 + pc
        slot = x * 16 + (z + (4 if far else 0)) % 8 * 2 + core
        return pltpu.make_async_remote_copy(
            src_ref=src.at[block],
            dst_ref=out_ref.at[slot],
            send_sem=send_sem.at[i + (40 if far else 0)],
            recv_sem=recv_sem.at[slot],
            device_id={SLAB[0]: px, SLAB[1]: pz, SLAB[2]: pc},
            device_id_type=pl.DeviceIdType.MESH,
        )

    def greet(i, carry):
        px, pz, pc, _ = peer(i)
        pl.semaphore_signal(
            barrier,
            inc=1,
            device_id={SLAB[0]: px, SLAB[1]: pz, SLAB[2]: pc},
            device_id_type=pl.DeviceIdType.MESH,
        )
        return carry

    locals_ = []
    for far in (False, True):
        src, reach = (far_ref, 1) if far else (own_ref, 2)
        slot = x * 16 + (z + (4 if far else 0)) % 8 * 2 + core
        locals_.append(
            pltpu.make_async_copy(
                src.at[(reach * 4 + x) * 2 + core], out_ref.at[slot], local_sem.at[int(far)]
            )
        )
        locals_[-1].start()
    barrier = pltpu.get_barrier_semaphore()
    lax.fori_loop(1, 40, greet, 0)
    pl.semaphore_wait(barrier, 39)

    def send(far):
        def body(i, carry):
            copy(i, far).start()
            return carry

        return body

    lax.fori_loop(24, 40, send(False), 0)
    lax.fori_loop(1, 24, send(False), 0)
    lax.fori_loop(1, 24, send(True), 0)

    def wait(far):
        def body(i, carry):
            px, pz, pc, dz = peer(i)
            one = copy(i, far)
            one.wait_send()
            slot = px * 16 + (pz + (4 if far else 0)) % 8 * 2 + pc
            pltpu.make_async_remote_copy(
                src_ref=own_ref.at[0],
                dst_ref=out_ref.at[slot],
                send_sem=send_sem.at[i],
                recv_sem=recv_sem.at[slot],
                device_id={SLAB[0]: px, SLAB[1]: pz, SLAB[2]: pc},
                device_id_type=pl.DeviceIdType.MESH,
            ).wait_recv()
            return carry

        return body

    lax.fori_loop(1, 40, wait(False), 0)
    lax.fori_loop(1, 24, wait(True), 0)
    for one in locals_:
        one.wait()


def spread(own, far):
    anywhere = pl.BlockSpec(memory_space=pl.ANY)
    return pl.pallas_call(
        spread_kernel,
        out_shape=jax.ShapeDtypeStruct((PEERS, 2, ROWS, COLS), F32),
        in_specs=[anywhere, anywhere],
        out_specs=anywhere,
        scratch_shapes=[
            pltpu.SemaphoreType.DMA((64,)),
            pltpu.SemaphoreType.DMA((PEERS,)),
            pltpu.SemaphoreType.DMA((2,)),
        ],
        compiler_params=pltpu.CompilerParams(collective_id=0, has_side_effects=True),
        name="spread",
    )(own.reshape(40, 2, ROWS, COLS), far.reshape(24, 2, ROWS, COLS))


STEPS = 8


def columns_kernel(
    x_ref,
    pr_ref,
    pi_ref,
    first_ref,
    first_lo_ref,
    second_ref,
    second_turn_ref,
    phase_ref,
    third_ref,
    fourth_ref,
    fourth_turn_ref,
    last_phase_ref,
    out_ref,
    held,
):
    step = pl.program_id(0)
    rows = x_ref.shape[1]
    per = pr_ref.shape[1]

    @pl.when(step < STEPS)
    def _():
        x = x_ref.reshape(128 * rows, COLS)
        for pair in range(rows // 2):
            values = jnp.concatenate(
                [x[pl.ds(2 * pair + e, 128, stride=rows), :] for e in range(2)], axis=1
            )
            high, low = split(values)
            both = jnp.concatenate([high, low], axis=0)
            result = mm(first_ref[...], both) + mm(first_lo_ref[...], high)
            for e in range(2):
                at = pl.multiple_of((step * rows + 2 * pair + e) * 256, 256)
                held[pl.ds(at, 256), :] = result[:, e * COLS : (e + 1) * COLS]

    @pl.when(jnp.logical_and(step >= STEPS, step < 2 * STEPS))
    def _():
        pr = pr_ref.reshape(64 * per, COLS)
        pi = pi_ref.reshape(64 * per, COLS)

        def body(i, carry):
            k = (step - STEPS) * per + i
            table = (
                second_ref[...] * phase_ref[k, 0:1, :] + second_turn_ref[...] * phase_ref[k, 1:2, :]
            )
            table_hi, table_lo = split(table)
            values = jnp.concatenate(
                [held[pl.ds(2 * k + s, 64, stride=256), :] for s in range(2)], axis=0
            )
            high, low = split(values)
            spectrum = mm(
                jnp.concatenate([table_hi, table_lo], axis=1),
                jnp.concatenate([high, high], axis=0),
            ) + mm(table_hi, low)
            re, im = spectrum[:64], spectrum[64:]
            psf_re = pr[pl.ds(i, 64, stride=per), :]
            psf_im = pi[pl.ds(i, 64, stride=per), :]
            filtered = jnp.concatenate(
                [re * psf_re - im * psf_im, re * psf_im + im * psf_re], axis=0
            )
            high, low = split(filtered)
            third = third_ref[...]
            result = mm(third, jnp.concatenate([high, high], axis=0)) + mm(third[:, :128], low)
            for s in range(2):
                held[pl.ds(2 * k + s, 64, stride=256), :] = result[64 * s : 64 * s + 64]
            return carry

        lax.fori_loop(0, per, body, 0, unroll=4)

    @pl.when(step >= 2 * STEPS)
    def _():
        out = out_ref.reshape(128 * rows, COLS)
        for pair in range(rows // 2):
            for e in range(2):
                row = (step - 2 * STEPS) * rows + 2 * pair + e
                table = (
                    fourth_ref[...] * last_phase_ref[row, 0:1, :]
                    + fourth_turn_ref[...] * last_phase_ref[row, 1:2, :]
                )
                table_hi, table_lo = split(table)
                at = pl.multiple_of(row * 256, 256)
                high, low = split(held[pl.ds(at, 256), :])
                full = mm(jnp.concatenate([table_hi, table_lo], axis=0), high)
                result = full[:128] + full[128:] + mm(table_hi, low)
                out[pl.ds(2 * pair + e, 128, stride=rows), :] = result


def columns(values, psf_re, psf_im):
    tables = column_tables()
    rows = ROWS // STEPS
    per = 128 // STEPS
    psf_re = psf_re.reshape(64, 128, COLS)
    psf_im = psf_im.reshape(64, 128, COLS)

    def psf_at(i):
        return (0, jnp.clip(i - STEPS, 0, STEPS - 1), 0)

    return pl.pallas_call(
        columns_kernel,
        out_shape=jax.ShapeDtypeStruct((128, ROWS, COLS), F32),
        grid=(3 * STEPS,),
        in_specs=[
            pl.BlockSpec((128, rows, COLS), lambda i: (0, jnp.minimum(i, STEPS - 1), 0)),
            pl.BlockSpec((64, per, COLS), psf_at),
            pl.BlockSpec((64, per, COLS), psf_at),
        ]
        + [whole(t.shape) for t in tables],
        out_specs=pl.BlockSpec(
            (128, rows, COLS), lambda i: (0, jnp.maximum(i - 2 * STEPS, 0), 0)
        ),
        scratch_shapes=[pltpu.VMEM((64 * 256, COLS), F32)],
        name="columns",
    )(values, psf_re, psf_im, *[jnp.asarray(t) for t in tables])


def inverse_kernel(
    y_ref, dirty_ref, first_ref, first_lo_ref, twr_ref, twi_ref, last_ref, out_ref, stat_ref, smear
):
    step = pl.program_id(0)
    rows = y_ref.shape[1]
    y = y_ref.reshape(128 * rows, COLS)
    for pair in range(rows // 2):
        values = jnp.concatenate(
            [y[pl.ds(2 * pair + e, 128, stride=rows), :] for e in range(2)], axis=1
        )
        high, low = split(values)
        partial = mm(first_ref[...], jnp.concatenate([high, low], axis=0)) + mm(
            first_lo_ref[...], high
        )
        turned = []
        for e in range(2):
            re = partial[:64, e * COLS : (e + 1) * COLS]
            im = partial[64:, e * COLS : (e + 1) * COLS]
            re = jnp.concatenate([re, re], axis=0)
            im = jnp.concatenate([im, im], axis=0)
            turned.append(
                jnp.concatenate(
                    [
                        re * twr_ref[...] - im * twi_ref[...],
                        re * twi_ref[...] + im * twr_ref[...],
                    ],
                    axis=1,
                )
            )
        high, low = split(jnp.concatenate(turned, axis=0))
        full = mm_nt(last_ref[...], high)
        result = full[:TILES] + full[TILES:] + mm_nt(last_ref[:TILES], low)
        for e in range(2):
            smear[pl.ds(2 * pair + e, TILES, stride=rows), :] = result[
                :, e * TILE_C : (e + 1) * TILE_C
            ]
    squares = jnp.zeros((rows, TILE_C), F32)
    peaks = jnp.zeros((rows, TILE_C), F32)
    for t in range(TILES):
        lanes = slice(t * TILE_C, (t + 1) * TILE_C)
        rest = dirty_ref[:, lanes] - smear[t * rows : (t + 1) * rows, :]
        out_ref[:, lanes] = rest
        squares += rest * rest
        peaks = jnp.maximum(peaks, jnp.abs(rest))

    @pl.when(step == 0)
    def _():
        stat_ref[...] = jnp.zeros_like(stat_ref)

    stat_ref[0:8, :] += squares
    stat_ref[8:16, :] = jnp.maximum(stat_ref[8:16, :], peaks)


def inverse_rows(values, dirty):
    tables = inverse_tables()
    rows = 8
    width = dirty.shape[1]
    return pl.pallas_call(
        inverse_kernel,
        out_shape=(
            jax.ShapeDtypeStruct((ROWS, width), F32),
            jax.ShapeDtypeStruct((16, TILE_C), F32),
        ),
        grid=(ROWS // rows,),
        in_specs=[
            pl.BlockSpec((128, rows, COLS), lambda i: (0, i, 0)),
            pl.BlockSpec((rows, width), lambda i: (i, 0)),
        ]
        + [whole(t.shape) for t in tables],
        out_specs=(
            pl.BlockSpec((rows, width), lambda i: (i, 0)),
            pl.BlockSpec((16, TILE_C), lambda i: (0, 0)),
        ),
        scratch_shapes=[pltpu.VMEM((TILES * rows, TILE_C), F32)],
        name="inverse",
    )(values, dirty, *[jnp.asarray(t) for t in tables])


def stats_kernel(pixels, own_ref, out_ref, mine, near, far, send_sem, recv_sem):
    chan = lax.axis_index("chan")
    x, z, core = (lax.axis_index(a) for a in SLAB)

    def near_peer(i):
        return (z + i // 2) % 8, (core + i) % 2

    def far_peer(i):
        return (chan + i // 4) % 4, (x + i) % 4

    mine[0] = jnp.concatenate(
        [
            jnp.sum(own_ref[:8], axis=0, keepdims=True),
            jnp.max(own_ref[8:], axis=0, keepdims=True),
            jnp.zeros((6, 128), F32),
        ],
        axis=0,
    )
    barrier = pltpu.get_barrier_semaphore()

    def greet(i, carry):
        pz, pc = near_peer(i)
        pl.semaphore_signal(
            barrier,
            inc=1,
            device_id={SLAB[1]: pz, SLAB[2]: pc},
            device_id_type=pl.DeviceIdType.MESH,
        )
        ph, px = far_peer(i)
        pl.semaphore_signal(
            barrier,
            inc=1,
            device_id={"chan": ph, SLAB[0]: px},
            device_id_type=pl.DeviceIdType.MESH,
        )
        return carry

    lax.fori_loop(1, 16, greet, 0)
    pl.semaphore_wait(barrier, 30)

    def near_copy(i, slot):
        pz, pc = near_peer(i)
        return pltpu.make_async_remote_copy(
            src_ref=mine.at[0],
            dst_ref=near.at[slot],
            send_sem=send_sem.at[i],
            recv_sem=recv_sem.at[slot],
            device_id={SLAB[1]: pz, SLAB[2]: pc},
            device_id_type=pl.DeviceIdType.MESH,
        )

    def far_copy(i, slot):
        ph, px = far_peer(i)
        return pltpu.make_async_remote_copy(
            src_ref=mine.at[1],
            dst_ref=far.at[slot],
            send_sem=send_sem.at[16 + i],
            recv_sem=recv_sem.at[16 + slot],
            device_id={"chan": ph, SLAB[0]: px},
            device_id_type=pl.DeviceIdType.MESH,
        )

    def swap(copy, slot, peer_slot, store):
        def start(i, carry):
            copy(i, slot).start()
            return carry

        def wait(i, carry):
            copy(i, slot).wait_send()
            copy(i, peer_slot(i)).wait_recv()
            return carry

        lax.fori_loop(1, 16, start, 0)
        store()
        lax.fori_loop(1, 16, wait, 0)

    def near_slot(i):
        pz, pc = near_peer(i)
        return pz * 2 + pc

    def far_slot(i):
        ph, px = far_peer(i)
        return ph * 4 + px

    def near_store():
        near[z * 2 + core] = mine[0]

    def far_store():
        far[chan * 4 + x] = mine[1]

    swap(near_copy, z * 2 + core, near_slot, near_store)
    total = near[0, 0:1]
    peak = near[0, 1:2]
    for i in range(1, 16):
        total = total + near[i, 0:1]
        peak = jnp.maximum(peak, near[i, 1:2])
    mine[1] = jnp.concatenate([total, peak, jnp.zeros((6, 128), F32)], axis=0)
    swap(far_copy, chan * 4 + x, far_slot, far_store)
    rows = []
    for c in range(4):
        total = far[4 * c, 0:1]
        peak = far[4 * c, 1:2]
        for i in range(1, 4):
            total = total + far[4 * c + i, 0:1]
            peak = jnp.maximum(peak, far[4 * c + i, 1:2])
        root = jnp.sqrt(jnp.sum(total, axis=1, keepdims=True) * (1.0 / pixels))
        rows.append(jnp.broadcast_to(root, (1, 128)))
        rows.append(jnp.broadcast_to(jnp.max(peak, axis=1, keepdims=True), (1, 128)))
    out_ref[...] = jnp.concatenate(rows, axis=0)


def statistics(own, pixels):
    inside = pl.BlockSpec(memory_space=pltpu.VMEM)
    out = pl.pallas_call(
        functools.partial(stats_kernel, pixels),
        out_shape=jax.ShapeDtypeStruct((8, 128), F32),
        in_specs=[inside],
        out_specs=inside,
        scratch_shapes=[
            pltpu.VMEM((2, 8, 128), F32),
            pltpu.VMEM((16, 8, 128), F32),
            pltpu.VMEM((16, 8, 128), F32),
            pltpu.SemaphoreType.DMA((32,)),
            pltpu.SemaphoreType.DMA((32,)),
        ],
        compiler_params=pltpu.CompilerParams(collective_id=1, has_side_effects=True),
        name="statistics",
    )(own)
    return out[0::2, 0], out[1::2, 0]


def boxes(flux, offsets, counts, dest_owner, dest_tile):
    blocks, slots = offsets.shape
    live = jnp.arange(slots, dtype=jnp.int32)[None, :] < counts[:, None]
    weights = jnp.where(live, flux, 0.0)
    places = (dest_tile[:, None] * (TILE_R * TILE_C) + offsets).astype(F32)
    payload = jnp.concatenate([places, weights], axis=1)
    owner = dest_owner[:, 0]
    ids = jnp.arange(blocks, dtype=jnp.int32)
    same = (owner[:, None] == owner[None, :]) & (ids[None, :] < ids[:, None])
    rank = jnp.sum(same.astype(jnp.int32), axis=1)
    slot = owner * 2 + rank
    marks = (slot[None, :] == jnp.arange(2 * PEERS, dtype=jnp.int32)[:, None]).astype(F32)
    box = jnp.dot(marks, payload, precision=lax.Precision.HIGHEST)
    box = box.reshape(4, 8, 2, 4, slots)
    return jnp.concatenate([box, jnp.roll(box, 4, axis=1)], axis=3).reshape(PEERS, 8, slots)


def on_device(flux, offsets, counts, dest_owner, dest_tile, dirty, psf_real, psf_imag):
    box = boxes(flux[0], offsets, counts, dest_owner, dest_tile)
    got = lax.all_to_all(box, SLAB, split_axis=0, concat_axis=0, tiled=True)
    tiles = got.reshape(PEERS, 2, 2, 2, -1)[:, :, :, 0, 0].astype(jnp.int32) // (TILE_R * TILE_C)
    tiles = (tiles + jnp.array([0, TILES], jnp.int32)[None, :, None]).reshape(-1)
    tiles = jnp.concatenate([tiles, lax.axis_index(SLAB[1])[None].astype(jnp.int32)])
    own, far = forward_rows(tiles, got.reshape(8 * PEERS, -1))
    turned = spread(own, far)
    back = columns(turned.reshape(2 * PEERS, ROWS, COLS), psf_real[0], psf_imag[0])
    back = back.reshape(PEERS, 2, ROWS, COLS)
    home = lax.all_to_all(back, SLAB, split_axis=0, concat_axis=0, tiled=True)
    residual, stats = inverse_rows(home.reshape(2 * PEERS, ROWS, COLS), dirty[0])
    pixels = PEERS * dirty.shape[1] * dirty.shape[2]
    rms_values, peak_values = statistics(stats, pixels)
    return residual[None], rms_values, peak_values


def solution(mesh):
    torus = Mesh(
        mesh.devices.reshape(mesh.shape["chan"], 4, 8, 2), ("chan", "slab_0", "slab_1", "slab_2")
    )
    in_specs = (
        P("chan", SLAB, None),
        P(SLAB, None),
        P(SLAB),
        P(SLAB, None),
        P(SLAB),
        P("chan", SLAB, None),
        P("chan", None, SLAB),
        P("chan", None, SLAB),
    )
    out_specs = (P("chan", SLAB, None), P(), P())
    return jax.shard_map(
        on_device, mesh=torus, in_specs=in_specs, out_specs=out_specs, check_vma=False
    )
```

```python
import functools
import math

import jax
import jax.numpy as jnp
import numpy as np
from jax import lax
from jax.experimental import pallas as pl
from jax.experimental.pallas import tpu as pltpu
from jax.sharding import Mesh
from jax.sharding import PartitionSpec as P

TILE_R = 64
TILE_C = 128
SLAB = ("slab_0", "slab_1", "slab_2")
ROWS = 64
COLS = 128
PEERS = 64
LENGTH = 8192
TILES = 32

BF = jnp.bfloat16
F32 = jnp.float32


def halves(table):
    table = np.asarray(table, np.float32)
    high = table.astype(jnp.bfloat16)
    low = (table - high.astype(np.float32)).astype(jnp.bfloat16)
    return high, low


def turns(first, second, length):
    return 2.0 * math.pi * (np.outer(first, second) % length) / length


def row_tables():
    j, tc, cc, d = np.arange(COLS), np.arange(TILES), np.arange(TILE_C), np.arange(PEERS)
    angle = turns(j, tc, 64)
    high, low = halves(np.concatenate([np.cos(angle), -np.sin(angle)], axis=0))
    first = np.concatenate([high, high, low], axis=1)
    angle = turns(j, cc, LENGTH)
    tw_re, tw_im = np.cos(angle).astype(np.float32), (-np.sin(angle)).astype(np.float32)
    d = d.reshape(4, 8, 2)[:, np.arange(12) % 8].transpose(1, 0, 2).reshape(-1)
    angle = turns(d, cc, 64)
    block = np.stack(
        [
            np.concatenate([np.cos(angle), np.sin(angle)], axis=1),
            np.concatenate([-np.sin(angle), np.cos(angle)], axis=1),
        ],
        axis=1,
    ).reshape(-1, 2 * TILE_C)
    return first, tw_re, tw_im, *halves(block)


def column_tables():
    a, k, m, b = np.arange(64), np.arange(128), np.arange(64), np.arange(64)
    angle = turns(k, a, 128)
    c, s = np.cos(angle), np.sin(angle)
    first = np.stack([np.stack([c, s], axis=2), np.stack([-s, c], axis=2)], axis=1)
    first_hi, first_lo = halves(first.reshape(256, 128))
    angle = turns(m, b, 64)
    c, s = np.cos(angle), np.sin(angle)
    second = np.block([[c, s], [-s, c]]).astype(np.float32)
    second_turn = np.block([[-s, c], [-c, -s]]).astype(np.float32)
    angle = turns(k, b, LENGTH)
    phase = np.stack([np.tile(np.cos(angle), (1, 2)), np.tile(np.sin(angle), (1, 2))], axis=1)
    angle = turns(b, m, 64)
    c, s = np.cos(angle), np.sin(angle)
    third_hi, third_lo = halves(np.block([[c, -s], [s, c]]))
    third = np.concatenate([third_hi, third_lo], axis=1)
    return (
        np.concatenate([first_hi, first_hi], axis=1),
        first_lo,
        second,
        second_turn,
        phase.astype(np.float32),
        third,
    )


def back_tables():
    r1, k, r0 = np.arange(64), np.arange(128), np.arange(64)
    angle = turns(r1, k, 128)
    c, s = np.cos(angle) * 2.0**-26, np.sin(angle) * 2.0**-26
    fourth = np.stack([np.stack([c, -s], axis=2), np.stack([s, c], axis=2)], axis=1)
    fourth_turn = np.stack([np.stack([-s, -c], axis=2), np.stack([c, -s], axis=2)], axis=1)
    angle = np.repeat(turns(r0, k, LENGTH), 2, axis=1)
    last_phase = np.stack([np.cos(angle), np.sin(angle)], axis=1)
    return (
        fourth.reshape(128, 256).astype(np.float32),
        fourth_turn.reshape(128, 256).astype(np.float32),
        last_phase.astype(np.float32),
    )


def inverse_tables():
    d, q, j, n2, n1 = np.arange(64), np.arange(64), np.arange(128), np.arange(128), np.arange(32)
    angle = turns(q, d, 64)
    c, s = np.cos(angle), np.sin(angle)
    first = np.concatenate(
        [
            np.stack([c, -s], axis=2).reshape(64, 128),
            np.stack([s, c], axis=2).reshape(64, 128),
        ],
        axis=0,
    )
    first_hi, first_lo = halves(first)
    angle = turns(n2, j, LENGTH)
    tw_re, tw_im = np.cos(angle).astype(np.float32), np.sin(angle).astype(np.float32)
    angle = turns(n1, j, 64)
    high, low = halves(np.concatenate([np.cos(angle), -np.sin(angle)], axis=1))
    return (
        np.concatenate([first_hi, first_hi], axis=1),
        first_lo,
        tw_re,
        tw_im,
        np.concatenate([high, low], axis=0),
    )


def split(value):
    high = value.astype(BF)
    low = (value - high.astype(F32)).astype(BF)
    return high, low


def mm(first, second):
    return jnp.dot(first, second, preferred_element_type=F32)


def mm_nt(first, second):
    return lax.dot_general(
        first, second, (((1,), (1,)), ((), ())), preferred_element_type=F32
    )


GROUP = 4


def rows_kernel(
    tile_ref, got_ref, first_ref, twr_ref, twi_ref, high_ref, low_ref, own_ref, far_ref, image
):
    step = pl.program_id(0)
    blocks = got_ref.shape[0] // 2
    rows = own_ref.shape[1]
    z = tile_ref[blocks]

    @pl.when(step == 0)
    def _():
        image[...] = jnp.zeros_like(image)
        row_ids = lax.broadcasted_iota(jnp.int32, (TILE_R, 128), 0)
        col_ids = lax.broadcasted_iota(jnp.int32, (TILE_C, 128), 0)

        def body(it, carry):
            tiles = []
            both = got_ref[pl.ds(pl.multiple_of(it * 2 * GROUP, 2 * GROUP), 2 * GROUP), :]
            for g in range(GROUP):
                place = both[2 * g : 2 * g + 1].astype(jnp.int32)
                flux = both[2 * g + 1 : 2 * g + 2]
                row = (place >> 7) & (TILE_R - 1)
                col = place & (TILE_C - 1)
                high = flux.astype(BF).astype(F32)
                low = flux - high
                here = row_ids == row
                lhs = jnp.concatenate(
                    [jnp.where(here, high, 0.0), jnp.where(here, low, 0.0)], axis=0
                ).astype(BF)
                rhs = jnp.where(col_ids == col, 1.0, 0.0).astype(BF)
                both_parts = mm_nt(lhs, rhs)
                tiles.append(both_parts[:TILE_R] + both_parts[TILE_R:])
            for g in range(GROUP):
                at = pl.ds(pl.multiple_of(tile_ref[it * GROUP + g] * TILE_R, TILE_R), TILE_R)
                image[at, :] += tiles[g]
            return carry

        lax.fori_loop(0, blocks // GROUP, body, 0)

    def chunk(base, reach, out_ref):
        many = (2 * reach + 1) * 16
        out = out_ref.reshape(many * rows, COLS)
        at = pl.ds(pl.multiple_of(lax.rem(z + 8 - reach, 8) * 16, 16), many)
        table_hi, table_lo = high_ref[at, :], low_ref[at, :]
        table = jnp.concatenate([table_hi, table_lo], axis=0)
        for pair in range(rows // 2):
            parts = []
            for e in range(2):
                x = image[pl.ds(base + 2 * pair + e, TILES, stride=TILE_R), :]
                high, low = split(x)
                parts.append(jnp.concatenate([high, low, high], axis=0))
            partial = mm(first_ref[...], jnp.concatenate(parts, axis=1))
            turned = []
            for e in range(2):
                re = partial[:COLS, e * TILE_C : (e + 1) * TILE_C]
                im = partial[COLS:, e * TILE_C : (e + 1) * TILE_C]
                turned.append(
                    jnp.concatenate(
                        [
                            re * twr_ref[...] - im * twi_ref[...],
                            re * twi_ref[...] + im * twr_ref[...],
                        ],
                        axis=1,
                    )
                )
            high, low = split(jnp.concatenate(turned, axis=0))
            full = mm_nt(table, high)
            result = full[:many] + full[many:] + mm_nt(table_hi, low)
            for e in range(2):
                out[pl.ds(2 * pair + e, many, stride=rows), :] = result[
                    :, e * COLS : (e + 1) * COLS
                ]

    chunks = ROWS // rows

    @pl.when(step < chunks)
    def _():
        chunk(step * rows, 2, own_ref)

    @pl.when(step >= chunks)
    def _():
        chunk(TILES * TILE_R + (step - chunks) * rows, 1, far_ref)


def whole(shape):
    return pl.BlockSpec(shape, lambda *_: (0,) * len(shape))


def forward_rows(tiles, got, rows=8):
    tables = row_tables()
    chunks = ROWS // rows
    return pl.pallas_call(
        rows_kernel,
        out_shape=(
            jax.ShapeDtypeStruct((80, ROWS, COLS), F32),
            jax.ShapeDtypeStruct((48, ROWS, COLS), F32),
        ),
        grid=(2 * chunks,),
        in_specs=[
            pl.BlockSpec(memory_space=pltpu.SMEM),
            whole(got.shape),
        ]
        + [whole(t.shape) for t in tables],
        out_specs=(
            pl.BlockSpec((80, rows, COLS), lambda i: (0, jnp.minimum(i, chunks - 1), 0)),
            pl.BlockSpec((48, rows, COLS), lambda i: (0, jnp.maximum(i - chunks, 0), 0)),
        ),
        scratch_shapes=[pltpu.VMEM((2 * TILES * TILE_R, TILE_C), F32)],
        name="rows",
    )(tiles, got, *[jnp.asarray(t) for t in tables])


def spread_kernel(own_ref, far_ref, out_ref, send_sem, recv_sem, local_sem):
    x, z, core = (lax.axis_index(a) for a in SLAB)

    def peer(i):
        order = i // 8
        dz = (order + 1) // 2 * (1 - 2 * (1 - order % 2) * jnp.minimum(order, 1))
        return (x + i // 2 % 4) % 4, (z + 8 + dz) % 8, (core + i) % 2, dz

    def copy(i, far):
        px, pz, pc, dz = peer(i)
        reach = 1 if far else 2
        src = far_ref if far else own_ref
        block = ((dz + reach) * 4 + px) * 2 + pc
        slot = x * 16 + (z + (4 if far else 0)) % 8 * 2 + core
        return pltpu.make_async_remote_copy(
            src_ref=src.at[block],
            dst_ref=out_ref.at[slot],
            send_sem=send_sem.at[i + (40 if far else 0)],
            recv_sem=recv_sem.at[slot],
            device_id={SLAB[0]: px, SLAB[1]: pz, SLAB[2]: pc},
            device_id_type=pl.DeviceIdType.MESH,
        )

    def greet(i, carry):
        px, pz, pc, _ = peer(i)
        pl.semaphore_signal(
            barrier,
            inc=1,
            device_id={SLAB[0]: px, SLAB[1]: pz, SLAB[2]: pc},
            device_id_type=pl.DeviceIdType.MESH,
        )
        return carry

    locals_ = []
    for far in (False, True):
        src, reach = (far_ref, 1) if far else (own_ref, 2)
        slot = x * 16 + (z + (4 if far else 0)) % 8 * 2 + core
        locals_.append(
            pltpu.make_async_copy(
                src.at[(reach * 4 + x) * 2 + core], out_ref.at[slot], local_sem.at[int(far)]
            )
        )
        locals_[-1].start()
    barrier = pltpu.get_barrier_semaphore()
    lax.fori_loop(1, 40, greet, 0)
    pl.semaphore_wait(barrier, 39)

    def send(far):
        def body(i, carry):
            copy(i, far).start()
            return carry

        return body

    lax.fori_loop(24, 40, send(False), 0)
    lax.fori_loop(1, 24, send(False), 0)
    lax.fori_loop(1, 24, send(True), 0)

    def wait(far):
        def body(i, carry):
            px, pz, pc, dz = peer(i)
            one = copy(i, far)
            one.wait_send()
            slot = px * 16 + (pz + (4 if far else 0)) % 8 * 2 + pc
            pltpu.make_async_remote_copy(
                src_ref=own_ref.at[0],
                dst_ref=out_ref.at[slot],
                send_sem=send_sem.at[i],
                recv_sem=recv_sem.at[slot],
                device_id={SLAB[0]: px, SLAB[1]: pz, SLAB[2]: pc},
                device_id_type=pl.DeviceIdType.MESH,
            ).wait_recv()
            return carry

        return body

    lax.fori_loop(1, 40, wait(False), 0)
    lax.fori_loop(1, 24, wait(True), 0)
    for one in locals_:
        one.wait()


def spread(own, far):
    anywhere = pl.BlockSpec(memory_space=pl.ANY)
    return pl.pallas_call(
        spread_kernel,
        out_shape=jax.ShapeDtypeStruct((PEERS, 2, ROWS, COLS), F32),
        in_specs=[anywhere, anywhere],
        out_specs=anywhere,
        scratch_shapes=[
            pltpu.SemaphoreType.DMA((64,)),
            pltpu.SemaphoreType.DMA((PEERS,)),
            pltpu.SemaphoreType.DMA((2,)),
        ],
        compiler_params=pltpu.CompilerParams(collective_id=0, has_side_effects=True),
        name="spread",
    )(own.reshape(40, 2, ROWS, COLS), far.reshape(24, 2, ROWS, COLS))


STEPS = 8
UNROLL = 4


def columns_kernel(
    x_ref,
    pr_ref,
    pi_ref,
    first_ref,
    first_lo_ref,
    second_ref,
    second_turn_ref,
    phase_ref,
    third_ref,
    out_ref,
    held,
):
    step = pl.program_id(0)
    rows = x_ref.shape[1]
    per = pr_ref.shape[1]

    @pl.when(step < STEPS)
    def _():
        x = x_ref.reshape(128 * rows, COLS)
        for pair in range(rows // 2):
            values = jnp.concatenate(
                [x[pl.ds(2 * pair + e, 128, stride=rows), :] for e in range(2)], axis=1
            )
            high, low = split(values)
            both = jnp.concatenate([high, low], axis=0)
            result = mm(first_ref[...], both) + mm(first_lo_ref[...], high)
            for e in range(2):
                at = pl.multiple_of((step * rows + 2 * pair + e) * 256, 256)
                held[pl.ds(at, 256), :] = result[:, e * COLS : (e + 1) * COLS]

    @pl.when(step >= STEPS)
    def _():
        pr = pr_ref.reshape(64 * per, COLS)
        pi = pi_ref.reshape(64 * per, COLS)

        out = out_ref.reshape(64 * 2 * per, COLS)

        def body(i, carry):
            k = (step - STEPS) * per + i
            table = (
                second_ref[...] * phase_ref[k, 0:1, :] + second_turn_ref[...] * phase_ref[k, 1:2, :]
            )
            table_hi, table_lo = split(table)
            values = jnp.concatenate(
                [held[pl.ds(2 * k + s, 64, stride=256), :] for s in range(2)], axis=0
            )
            high, low = split(values)
            spectrum = mm(
                jnp.concatenate([table_hi, table_lo], axis=1),
                jnp.concatenate([high, high], axis=0),
            ) + mm(table_hi, low)
            re, im = spectrum[:64], spectrum[64:]
            psf_re = pr[pl.ds(i, 64, stride=per), :]
            psf_im = pi[pl.ds(i, 64, stride=per), :]
            filtered = jnp.concatenate(
                [re * psf_re - im * psf_im, re * psf_im + im * psf_re], axis=0
            )
            high, low = split(filtered)
            third = third_ref[...]
            result = mm(third, jnp.concatenate([high, high], axis=0)) + mm(third[:, :128], low)
            for s in range(2):
                out[pl.ds(2 * i + s, 64, stride=2 * per), :] = result[64 * s : 64 * s + 64]
            return carry

        lax.fori_loop(0, per, body, 0, unroll=UNROLL)


def columns(values, psf_re, psf_im):
    tables = column_tables()
    rows = ROWS // STEPS
    per = 128 // STEPS
    psf_re = psf_re.reshape(64, 128, COLS)
    psf_im = psf_im.reshape(64, 128, COLS)

    def later(i):
        return (0, jnp.maximum(i - STEPS, 0), 0)

    return pl.pallas_call(
        columns_kernel,
        out_shape=jax.ShapeDtypeStruct((64, 256, COLS), F32),
        grid=(2 * STEPS,),
        in_specs=[
            pl.BlockSpec((128, rows, COLS), lambda i: (0, jnp.minimum(i, STEPS - 1), 0)),
            pl.BlockSpec((64, per, COLS), later),
            pl.BlockSpec((64, per, COLS), later),
        ]
        + [whole(t.shape) for t in tables],
        out_specs=pl.BlockSpec((64, 2 * per, COLS), later),
        scratch_shapes=[pltpu.VMEM((64 * 256, COLS), F32)],
        name="columns",
    )(values, psf_re, psf_im, *[jnp.asarray(t) for t in tables])


CHUNKS = 4
PART = ROWS // CHUNKS
MESH = pl.DeviceIdType.MESH


def back_kernel(
    pixels,
    v_ref,
    dirty_ref,
    fourth_ref,
    fourth_turn_ref,
    last_phase_ref,
    first_ref,
    first_lo_ref,
    twr_ref,
    twi_ref,
    last_ref,
    out_ref,
    rms_ref,
    peak_ref,
    v_buf,
    y_buf,
    in_buf,
    smear,
    mine,
    near,
    far,
    v_sem,
    send_sem,
    recv_sem,
    own_sem,
    near_send,
    near_recv,
    far_send,
    far_recv,
):
    chan = lax.axis_index("chan")
    x, z, core = (lax.axis_index(a) for a in SLAB)
    me = x * 16 + z * 2 + core
    fetches = [
        pltpu.make_async_copy(v_ref.at[pl.ds(c * PART, PART)], v_buf.at[c], v_sem.at[c])
        for c in range(CHUNKS)
    ]
    for fetch in fetches:
        fetch.start()
    barrier = pltpu.get_barrier_semaphore()

    def peer(i):
        turn = i % 8
        dz = (turn + 1) // 2 * (1 - 2 * (1 - turn % 2)) + 8
        return (x + i // 16) % 4, (z + dz) % 8, (core + i // 8) % 2

    def where(i):
        px, pz, pc = peer(i)
        return {SLAB[0]: px, SLAB[1]: pz, SLAB[2]: pc}

    def greet(i, carry):
        pl.semaphore_signal(barrier, inc=1, device_id=where(i), device_id_type=MESH)
        return carry

    def far_peer(i):
        return (chan + 1 + i // 4) % 4, (x + i) % 4

    def greet_far(i, carry):
        ph, px = far_peer(i)
        pl.semaphore_signal(
            barrier, inc=1, device_id={"chan": ph, SLAB[0]: px}, device_id_type=MESH
        )
        return carry

    lax.fori_loop(1, PEERS, greet, 0)
    lax.fori_loop(0, 12, greet_far, 0)

    def produce(c):
        def body(g, carry):
            for e in range(4):
                i = g * 4 + e
                table = (
                    fourth_ref[...] * last_phase_ref[c * PART + i, 0:1, :]
                    + fourth_turn_ref[...] * last_phase_ref[c * PART + i, 1:2, :]
                )
                table_hi, table_lo = split(table)
                high, low = split(v_buf[c, i])
                full = mm(jnp.concatenate([table_hi, table_lo], axis=0), high)
                result = full[:128] + full[128:] + mm(table_hi, low)
                y_buf[c, pl.ds(i, 128, stride=PART), :] = result
            return carry

        fetches[c].wait()
        lax.fori_loop(0, PART // 4, body, 0)

    span = 2 * PART

    def block(slot):
        return pl.ds(pl.multiple_of(slot * span, span), span)

    def send(c):
        pltpu.make_async_copy(
            y_buf.at[c, block(me)], in_buf.at[c, block(me)], own_sem.at[c]
        ).start()

        def body(i, carry):
            px, pz, pc = peer(i)
            pltpu.make_async_remote_copy(
                src_ref=y_buf.at[c, block(px * 16 + pz * 2 + pc)],
                dst_ref=in_buf.at[c, block(me)],
                send_sem=send_sem.at[c],
                recv_sem=recv_sem.at[c],
                device_id=where(i),
                device_id_type=MESH,
            ).start()
            return carry

        lax.fori_loop(1, PEERS, body, 0)

    def collect(c):
        others = pl.ds(0, (PEERS - 1) * span)
        pltpu.make_async_copy(
            in_buf.at[c, others], in_buf.at[c, others], recv_sem.at[c]
        ).wait()
        pltpu.make_async_copy(
            y_buf.at[c, block(me)], in_buf.at[c, block(me)], own_sem.at[c]
        ).wait()

    def consume(c):
        def body(pair, carry):
            values = jnp.concatenate(
                [in_buf[c, pl.ds(2 * pair + e, 128, stride=PART), :] for e in range(2)], axis=1
            )
            high, low = split(values)
            partial = mm(first_ref[...], jnp.concatenate([high, low], axis=0)) + mm(
                first_lo_ref[...], high
            )
            turned = []
            for e in range(2):
                re = partial[:64, e * COLS : (e + 1) * COLS]
                im = partial[64:, e * COLS : (e + 1) * COLS]
                re = jnp.concatenate([re, re], axis=0)
                im = jnp.concatenate([im, im], axis=0)
                turned.append(
                    jnp.concatenate(
                        [
                            re * twr_ref[...] - im * twi_ref[...],
                            re * twi_ref[...] + im * twr_ref[...],
                        ],
                        axis=1,
                    )
                )
            high, low = split(jnp.concatenate(turned, axis=0))
            full = mm_nt(last_ref[...], high)
            result = full[:TILES] + full[TILES:] + mm_nt(last_ref[:TILES], low)
            for e in range(2):
                smear[pl.ds(2 * pair + e, TILES, stride=PART), :] = result[
                    :, e * TILE_C : (e + 1) * TILE_C
                ]
            return carry

        lax.fori_loop(0, PART // 2, body, 0, unroll=2)
        squares = jnp.zeros((PART, TILE_C), F32)
        peaks = jnp.zeros((PART, TILE_C), F32)
        for t in range(TILES):
            at = (slice(c * PART, (c + 1) * PART), slice(t * TILE_C, (t + 1) * TILE_C))
            rest = dirty_ref[at] - smear[t * PART : (t + 1) * PART, :]
            out_ref[at] = rest
            squares += rest * rest
            peaks = jnp.maximum(peaks, jnp.abs(rest))
        return (
            jnp.sum(squares, axis=0, keepdims=True),
            jnp.max(peaks, axis=0, keepdims=True),
        )

    produce(0)
    pl.semaphore_wait(barrier, PEERS - 1 + 12)
    send(0)
    for c in range(1, CHUNKS):
        produce(c)
        if c > 1:
            send(c - 1)
    collect(0)
    send(CHUNKS - 1)
    total, peak = consume(0)
    for c in range(1, CHUNKS):
        collect(c)
        one, top = consume(c)
        total, peak = total + one, jnp.maximum(peak, top)
    for c in range(CHUNKS):
        others = pl.ds(0, (PEERS - 1) * span)
        pltpu.make_async_copy(y_buf.at[c, others], y_buf.at[c, others], send_sem.at[c]).wait()

    filler = jnp.zeros((6, 128), F32)
    mine[0] = jnp.concatenate([total, peak, filler], axis=0)

    def near_copy(i, slot):
        return pltpu.make_async_remote_copy(
            src_ref=mine.at[0],
            dst_ref=near.at[slot],
            send_sem=near_send.at[i],
            recv_sem=near_recv.at[slot],
            device_id={SLAB[1]: (z + i // 2) % 8, SLAB[2]: (core + i) % 2},
            device_id_type=MESH,
        )

    def far_copy(i, slot):
        return pltpu.make_async_remote_copy(
            src_ref=mine.at[1],
            dst_ref=far.at[slot],
            send_sem=far_send.at[i],
            recv_sem=far_recv.at[slot],
            device_id={"chan": (chan + i // 4) % 4, SLAB[0]: (x + i) % 4},
            device_id_type=MESH,
        )

    def near_slot(i):
        return (z + i // 2) % 8 * 2 + (core + i) % 2

    def far_slot(i):
        return (chan + i // 4) % 4 * 4 + (x + i) % 4

    def swap(copy, slot_of):
        def start(i, carry):
            copy(i, slot_of(0)).start()
            return carry

        lax.fori_loop(1, 16, start, 0)

    def settle(copy, slot_of):
        def wait(i, carry):
            copy(i, slot_of(0)).wait_send()
            copy(i, slot_of(i)).wait_recv()
            return carry

        lax.fori_loop(1, 16, wait, 0)

    swap(near_copy, near_slot)
    near[near_slot(0)] = mine[0]
    settle(near_copy, near_slot)
    total = near[0, 0:1]
    peak = near[0, 1:2]
    for i in range(1, 16):
        total = total + near[i, 0:1]
        peak = jnp.maximum(peak, near[i, 1:2])
    mine[1] = jnp.concatenate([total, peak, filler], axis=0)
    swap(far_copy, far_slot)
    far[far_slot(0)] = mine[1]
    settle(far_copy, far_slot)
    lane = lax.broadcasted_iota(jnp.int32, (1, 128), 1)
    roots = jnp.zeros((1, 128), F32)
    tops = jnp.zeros((1, 128), F32)
    for h in range(4):
        total = far[4 * h, 0:1]
        peak = far[4 * h, 1:2]
        for i in range(1, 4):
            total = total + far[4 * h + i, 0:1]
            peak = jnp.maximum(peak, far[4 * h + i, 1:2])
        mean = jnp.sum(total, axis=1, keepdims=True) * (1.0 / pixels)
        roots = jnp.where(lane == h, jnp.sqrt(mean), roots)
        tops = jnp.where(lane == h, jnp.max(peak, axis=1, keepdims=True), tops)
    rms_ref[...] = roots
    peak_ref[...] = tops


def back(values, dirty, pixels):
    tables = back_tables() + inverse_tables()
    inside = pl.BlockSpec(memory_space=pltpu.VMEM)
    residual, rms, peaks = pl.pallas_call(
        functools.partial(back_kernel, pixels),
        out_shape=(
            jax.ShapeDtypeStruct(dirty.shape, F32),
            jax.ShapeDtypeStruct((1, 128), F32),
            jax.ShapeDtypeStruct((1, 128), F32),
        ),
        in_specs=[pl.BlockSpec(memory_space=pl.ANY)] + [inside] * (1 + len(tables)),
        out_specs=(inside, inside, inside),
        scratch_shapes=[
            pltpu.VMEM((CHUNKS, PART, 256, COLS), F32),
            pltpu.VMEM((CHUNKS, 2 * PEERS * PART, COLS), F32),
            pltpu.VMEM((CHUNKS, 2 * PEERS * PART, COLS), F32),
            pltpu.VMEM((TILES * PART, TILE_C), F32),
            pltpu.VMEM((2, 8, 128), F32),
            pltpu.VMEM((16, 8, 128), F32),
            pltpu.VMEM((16, 8, 128), F32),
            pltpu.SemaphoreType.DMA((CHUNKS,)),
            pltpu.SemaphoreType.DMA((CHUNKS,)),
            pltpu.SemaphoreType.DMA((CHUNKS,)),
            pltpu.SemaphoreType.DMA((CHUNKS,)),
            pltpu.SemaphoreType.DMA((16,)),
            pltpu.SemaphoreType.DMA((16,)),
            pltpu.SemaphoreType.DMA((16,)),
            pltpu.SemaphoreType.DMA((16,)),
        ],
        compiler_params=pltpu.CompilerParams(collective_id=1, has_side_effects=True),
        name="back",
    )(values, dirty, *[jnp.asarray(t) for t in tables])
    return residual, rms[0, :4], peaks[0, :4]


def boxes(flux, offsets, counts, dest_owner, dest_tile):
    blocks, slots = offsets.shape
    live = jnp.arange(slots, dtype=jnp.int32)[None, :] < counts[:, None]
    weights = jnp.where(live, flux, 0.0)
    places = (dest_tile[:, None] * (TILE_R * TILE_C) + offsets).astype(F32)
    payload = jnp.concatenate([places, weights], axis=1)
    owner = dest_owner[:, 0]
    ids = jnp.arange(blocks, dtype=jnp.int32)
    same = (owner[:, None] == owner[None, :]) & (ids[None, :] < ids[:, None])
    rank = jnp.sum(same.astype(jnp.int32), axis=1)
    slot = owner * 2 + rank
    marks = (slot[None, :] == jnp.arange(2 * PEERS, dtype=jnp.int32)[:, None]).astype(F32)
    box = jnp.dot(marks, payload, precision=lax.Precision.HIGHEST)
    box = box.reshape(4, 8, 2, 4, slots)
    return jnp.concatenate([box, jnp.roll(box, 4, axis=1)], axis=3).reshape(PEERS, 8, slots)


def on_device(flux, offsets, counts, dest_owner, dest_tile, dirty, psf_real, psf_imag):
    box = boxes(flux[0], offsets, counts, dest_owner, dest_tile)
    got = lax.all_to_all(box, SLAB, split_axis=0, concat_axis=0, tiled=True)
    tiles = got.reshape(PEERS, 2, 2, 2, -1)[:, :, :, 0, 0].astype(jnp.int32) // (TILE_R * TILE_C)
    tiles = (tiles + jnp.array([0, TILES], jnp.int32)[None, :, None]).reshape(-1)
    tiles = jnp.concatenate([tiles, lax.axis_index(SLAB[1])[None].astype(jnp.int32)])
    own, far = forward_rows(tiles, got.reshape(8 * PEERS, -1))
    turned = spread(own, far)
    values = columns(turned.reshape(2 * PEERS, ROWS, COLS), psf_real[0], psf_imag[0])
    pixels = PEERS * dirty.shape[1] * dirty.shape[2]
    residual, rms_values, peak_values = back(values, dirty[0], pixels)
    return residual[None], rms_values, peak_values


def solution(mesh):
    torus = Mesh(
        mesh.devices.reshape(mesh.shape["chan"], 4, 8, 2), ("chan", "slab_0", "slab_1", "slab_2")
    )
    in_specs = (
        P("chan", SLAB, None),
        P(SLAB, None),
        P(SLAB),
        P(SLAB, None),
        P(SLAB),
        P("chan", SLAB, None),
        P("chan", None, SLAB),
        P("chan", None, SLAB),
    )
    out_specs = (P("chan", SLAB, None), P(), P())
    return jax.shard_map(
        on_device, mesh=torus, in_specs=in_specs, out_specs=out_specs, check_vma=False
    )
```
